128 devices in a mesh: dp: 16 (over z, y), expert: 8 (over x, core).
Axes of the slice: x: 4, y: 4, z: 4, core: 2. Of those that a mesh axis runs over, the one named last changes fastest.
Arguments:
- tokens: bfloat16 [2048, 4096], P('dp'), may hold values from -6 to 6
- expert_ids: int32 [2048, 2], P('dp'), may hold values from 0 to 7, all different within a row; in each aligned block of 128 rows (0 to 127, 128 to 255, ...) at most 96 rows name the same one
- gate_weights: float32 [2048, 2], P('dp'), may hold values from 0.2 to 1
- live_counts: int32 [16], P('dp'), may hold values from 64 to 128, as said below
- w_gate: bfloat16 [8, 4096, 8192], P('expert', None, 'dp'), may hold values from -0.09375 to 0.09375
- w_up: bfloat16 [8, 4096, 8192], P('expert', None, 'dp'), may hold values from -0.09375 to 0.09375
- w_down: bfloat16 [8, 8192, 4096], P('expert', 'dp'), may hold values from -0.0625 to 0.0625
Outputs:
- mixed: bfloat16 [2048, 4096], P('dp')
- total_loads: int32 [8], replicated
The draws below stay inside these ranges and needn't reach their ends.
Inputs may be any that keep to these rules, and one draw needn't show every extreme that they name: `expert_ids`: each token names two different experts. Among the tokens of one rank no expert is named more than 96 times, a bound that some block reaches in some ranks. Rank r's first live_counts[r] tokens are live, the rest are padding. Some rank has all 128 tokens live.
All inputs are finite; a program needn't handle non-finite values.
Results may differ from the reference program's by a relative error of at most 0.017.
Values may be sent and summed in bfloat16 or wider, within the bound.
No kernel may reach another device: no remote copies, remote signals or barrier semaphores. Data moves between devices by JAX's collectives and lax.ppermute only.
A program may use at most 128 MiB of HBM per device.

```python
import math
import jax
import jax.numpy as jnp
import numpy as np
from jax import lax

D = 4096
FF = 8192
TOK_DEV = 128
EXPERTS = 8
CAP = 96
RANKS = 16
TOKENS = 2048
N_DP = 16


def draw_live_counts(key, part):
    base = jax.random.fold_in(key, 11)
    first_key, second_key = jax.random.split(base)
    counts = jax.random.randint(first_key, (RANKS,), TOK_DEV // 2, TOK_DEV + 1)
    full_rank = jax.random.randint(second_key, (), 0, RANKS)
    return jnp.where(jnp.arange(RANKS) == full_rank, TOK_DEV, counts).astype(jnp.int32)


def shard_levels(rng, dims, cuts, smallest, high):
    loudness = 1.0
    for axis_at, blocks in cuts:
        draws = jax.random.uniform(jax.random.fold_in(jax.random.fold_in(rng, 6), axis_at), (blocks,), jnp.float32, smallest / len(cuts), high / len(cuts))
        loudness = loudness * jnp.repeat(jnp.exp(draws), dims[axis_at] // blocks).reshape((-1,) + (1,) * (len(dims) - 1 - axis_at))
    return loudness


def shared_out(rng, own, number, rows, count, top, bound, slope):
    ranking = jax.random.permutation(rng, count)
    packed, usual = load_shares(count, rows * top, bound, slope, True), load_shares(count, rows * top, bound, slope, False)
    places = jnp.arange(count)

    def named(sizes, offset_by):
        used = int((sizes > 0).sum())
        fixed = max(1, used // 4)
        passed = fixed + (places - fixed + offset_by * (used - fixed)) % max(1, count - fixed)
        return jnp.zeros((count,), jnp.int32).at[ranking[jnp.where(places < fixed, places, passed)]].set(jnp.asarray(sizes, jnp.int32))

    sizes = jnp.where(number % 4 == 0, named(packed, number // 4), named(usual, number - number // 4 - 1))
    mixed = jax.random.permutation(jax.random.fold_in(own, 3), count)
    donor, receiver = mixed[0:count // 2 * 2:2], mixed[1:count // 2 * 2:2]
    margin = jnp.minimum(sizes[donor] - 1, bound - sizes[receiver]) // 2
    margin = jnp.where((donor == ranking[0]) | (receiver == ranking[0]) | (sizes[receiver] == 0), 0, jnp.maximum(margin, 0))
    passed = jax.random.randint(jax.random.fold_in(own, 4), (count // 2,), 0, 1 << 20) % (margin + 1)
    sizes = sizes.at[donor].add(-passed).at[receiver].add(passed)
    items = jnp.searchsorted(jnp.cumsum(sizes), jnp.arange(rows * top), side="right").astype(jnp.int32)
    grid = items.reshape(top, rows).T
    grid = grid[jax.random.permutation(jax.random.fold_in(own, 1), rows)]
    offset_by = jax.random.randint(jax.random.fold_in(own, 2), (rows, 1), 0, top)
    return jnp.take_along_axis(grid, (jnp.arange(top)[None, :] + offset_by) % top, axis=1)


def load_shares(amount, total, bound, lean, full):
    portions = [(1 << 20) // math.isqrt(standing ** lean) + 1 for standing in range(1, amount + 1)]
    largest = bound if full else min(bound, max(-(-total // amount), total * portions[0] // sum(portions)))
    least = 1 if total - largest >= amount - 1 else 0
    given, spare = [largest] + [least] * (amount - 1), total - largest - least * (amount - 1)
    while spare > 0:
        movable = [i for i in range(1, amount) if given[i] < largest] or [i for i in range(1, amount) if given[i] < bound]
        whole, left = sum([portions[i] for i in movable]), spare
        for i in movable:
            more = min(bound - given[i], max(1, left * portions[i] // whole), spare)
            given[i] = given[i] + more
            spare = spare - more
    return np.array(given)


def gaussian(own_key, extent, width, bound, pieces=(), held_as=jnp.bfloat16):
    result = width * jax.random.normal(own_key, extent, jnp.float32)
    if pieces:
        result = result * shard_levels(own_key, extent, pieces, -0.22, 0.18)
    return jnp.clip(result, -bound, bound).astype(held_as)


def setup_inputs(seed: int = 0) -> dict:
    streams_of = jax.random.split(jax.random.key(seed), 8)
    tokens = gaussian(streams_of[0], (TOKENS, D), 1.0, 6.0, ((0, 16),))
    expert_ids_keys = jax.random.split(jax.random.fold_in(streams_of[1], 1), TOKENS // TOK_DEV)
    expert_ids_turns = jax.random.permutation(jax.random.fold_in(streams_of[1], 3), TOKENS // TOK_DEV)
    expert_ids = jax.vmap(lambda own, number: shared_out(jax.random.fold_in(streams_of[1], 2), own, number, TOK_DEV, EXPERTS, 2, CAP, 2))(expert_ids_keys, expert_ids_turns).reshape((TOKENS, 2))
    gate_weights = jnp.clip(0.2 + 0.8 * jax.random.uniform(streams_of[2], (TOKENS, 2), jnp.float32) ** shard_levels(streams_of[2], (TOKENS, 2), ((0, 16),), -0.2, 0.2), 0.2, 1.0)
    live_counts = draw_live_counts(jax.random.fold_in(streams_of[7], 71), 0)
    w_gate = gaussian(streams_of[4], (EXPERTS, D, FF), D ** -0.5, 0.09375, ((0, 8), (2, 16)))
    w_up = gaussian(streams_of[5], (EXPERTS, D, FF), D ** -0.5, 0.09375, ((0, 8), (2, 16)))
    w_down = gaussian(streams_of[6], (EXPERTS, FF, D), FF ** -0.5, 0.0625, ((0, 8), (1, 16)))
    return {"tokens": tokens, "expert_ids": expert_ids, "gate_weights": gate_weights, "live_counts": live_counts, "w_gate": w_gate, "w_up": w_up, "w_down": w_down}


def plan_routes(expert_ids, live_total, n_experts, capacity):
    row_count = expert_ids.shape[0]
    is_live = jnp.arange(row_count, dtype=jnp.int32) < live_total
    flat_ids = expert_ids.reshape(-1)
    live_pairs = jnp.repeat(is_live, 2)
    one_hot = ((flat_ids[:, None] == jnp.arange(n_experts, dtype=jnp.int32)[None, :]) & live_pairs[:, None]).astype(jnp.int32)
    earlier = jnp.cumsum(one_hot, axis=0) - one_hot
    slot_index = jnp.sum(earlier * one_hot, axis=1)
    targets = jnp.where(live_pairs, flat_ids * capacity + slot_index, -1).astype(jnp.int32)
    return targets.reshape(row_count, 2), jnp.sum(one_hot, axis=0)


def dispatch_rows(tokens, targets, slots_all):
    wanted = targets.reshape(-1)[None, :] == jnp.arange(slots_all, dtype=jnp.int32)[:, None]
    wanted = jnp.any(wanted.reshape(slots_all, -1, 2), axis=2).astype(jnp.bfloat16)
    return jnp.dot(wanted, tokens, preferred_element_type=jnp.float32).astype(jnp.bfloat16)


def combine_rows(results, targets, gate_weights):
    pick_index = jnp.maximum(targets, 0).astype(jnp.int32)
    selected = results[pick_index].astype(jnp.float32)
    weights = jnp.where(targets >= 0, gate_weights, jnp.zeros_like(gate_weights))
    return jnp.sum(weights[:, :, None] * selected, axis=1).astype(jnp.bfloat16)


def reference(tokens, expert_ids, gate_weights, live_counts, w_gate, w_up, w_down):
    tok_blocks = tokens.reshape(RANKS, TOK_DEV, D)
    id_blocks = expert_ids.reshape(RANKS, TOK_DEV, 2)
    gate_blocks = gate_weights.reshape(RANKS, TOK_DEV, 2)
    targets, loads = jax.vmap(lambda ids, live: plan_routes(ids, live, EXPERTS, CAP))(id_blocks, live_counts)
    outbound = jax.vmap(lambda toks, tgt: dispatch_rows(toks, tgt, EXPERTS * CAP))(tok_blocks, targets)
    per_expert = outbound.reshape(RANKS, EXPERTS, CAP, D).transpose(1, 0, 2, 3).reshape(EXPERTS, RANKS * CAP, D)
    shard_width = FF // N_DP

    def run_expert(operands):
        row_block, gate_matrix, up_matrix, down_matrix = operands
        total = jnp.zeros((row_block.shape[0], D), jnp.float32)
        for shard_index in range(N_DP):
            lower = shard_index * shard_width
            gate_act = jnp.dot(row_block, gate_matrix[:, lower:lower + shard_width], preferred_element_type=jnp.float32)
            up_act = jnp.dot(row_block, up_matrix[:, lower:lower + shard_width], preferred_element_type=jnp.float32)
            hidden = (jax.nn.silu(gate_act) * up_act).astype(jnp.bfloat16)
            partial_term = jnp.dot(hidden, down_matrix[lower:lower + shard_width, :], preferred_element_type=jnp.float32).astype(jnp.bfloat16)
            partial_term = lax.optimization_barrier(partial_term)
            total = total + partial_term.astype(jnp.float32)
        return total.astype(jnp.bfloat16)

    results = lax.map(run_expert, (per_expert, w_gate, w_up, w_down))
    returned = results.reshape(EXPERTS, RANKS, CAP, D).transpose(1, 0, 2, 3).reshape(RANKS, EXPERTS * CAP, D)
    mixed = jax.vmap(combine_rows)(returned, targets, gate_blocks).reshape(TOKENS, D)
    return mixed, jnp.sum(loads, axis=0).astype(jnp.int32)
```

```python
import jax
import jax.numpy as jnp
from jax import lax
from jax.sharding import Mesh
from jax.sharding import PartitionSpec as P

DP = ("z", "y")
PLANE = ("z", "y", "c")


def plane_perm(stage, shift, nz, ny):
    pairs = []
    for z in range(nz):
        for y in range(ny):
            for c in range(2):
                along_y = (stage == 1) == (c == 0)
                to_z, to_y = (z, (y + shift) % ny) if along_y else ((z + shift) % nz, y)
                pairs.append(((z * ny + y) * 2 + c, (to_z * ny + to_y) * 2 + c))
    return pairs


def hop(value, stage, shift):
    perm = plane_perm(stage, shift, lax.axis_size("z"), lax.axis_size("y"))
    return lax.ppermute(value, PLANE, perm)


def swap(value):
    return lax.ppermute(value, "c", [(0, 1), (1, 0)])


def x_hop(value, shift):
    size = lax.axis_size("x")
    return lax.ppermute(value, "x", [(i, (i + shift) % size) for i in range(size)])


def ring_gather(value, stage):
    half = value.shape[0] // 2
    ahead = hop(value, stage, -1)
    behind = hop(value, stage, 1)
    far_low = hop(behind[:half], stage, 1)
    far_high = hop(ahead[half:], stage, -1)
    return [value, ahead, behind, far_low, far_high]


def add(a, b):
    return (a.astype(jnp.float32) + b.astype(jnp.float32)).astype(jnp.bfloat16)


def ring_reduce(blocks, stage):
    mine, ahead, behind, far_low, far_high = blocks
    half = mine.shape[0] // 2
    got_low = hop(far_low, stage, 1)
    got_high = hop(far_high, stage, -1)
    ahead = jnp.concatenate([add(ahead[:half], got_low), ahead[half:]])
    behind = jnp.concatenate([behind[:half], add(behind[half:], got_high)])
    a = hop(ahead, stage, 1)
    b = hop(behind, stage, -1)
    total = mine.astype(jnp.float32) + a.astype(jnp.float32) + b.astype(jnp.float32)
    return total.astype(jnp.bfloat16)


def direct_gather(value, stage):
    return [value, hop(value, stage, -1), hop(value, stage, 1), hop(value, stage, 2)]


def per_device(tokens, expert_ids, gate_weights, live_counts, w_gate, w_up, w_down):
    core = lax.axis_index("c")
    x_at = lax.axis_index("x")
    n_x = lax.axis_size("x")
    my_expert = x_at * 2 + core
    n_experts = n_x * 2
    rows = tokens.shape[0] // 2
    start = core * rows

    def my_half(array):
        return lax.dynamic_slice_in_dim(array, start, rows, 0)

    is_live = (start + jnp.arange(rows, dtype=jnp.int32) < live_counts[0]).astype(jnp.float32)
    routes = jnp.concatenate(
        [my_half(expert_ids).astype(jnp.float32).T, my_half(gate_weights).T, is_live[None], jnp.zeros((3, rows))]
    )
    near = jnp.stack(direct_gather(routes, 1))
    routes = jnp.stack(direct_gather(near, 2))
    routes_other = swap(routes)

    def weight_of(route):
        named = (route[..., 0:2, :] == my_expert.astype(jnp.float32)) & (route[..., 4:5, :] > 0)
        return jnp.sum(jnp.where(named, route[..., 2:4, :], 0.0), axis=-2)

    def loads_of(route):
        ids = route[..., 0:2, :]
        live = route[..., 4:5, :] > 0
        experts = jnp.arange(n_experts, dtype=jnp.float32).reshape(-1, 1, 1, 1, 1)
        return jnp.sum(((ids[None] == experts) & live[None]).astype(jnp.int32), axis=(1, 2, 3, 4))

    total_loads = loads_of(routes) + loads_of(routes_other)
    weights = weight_of(routes).reshape(4, 4 * rows)
    weights_other = weight_of(routes_other).reshape(4, 4 * rows)

    gate_matrix = w_gate[0]
    up_matrix = w_up[0]
    down_matrix = w_down[0]

    def expert(block, weight):
        gate_act = jnp.dot(block, gate_matrix, preferred_element_type=jnp.float32)
        up_act = jnp.dot(block, up_matrix, preferred_element_type=jnp.float32)
        hidden = (jax.nn.silu(gate_act) * up_act).astype(jnp.bfloat16)
        out = jnp.dot(hidden, down_matrix, preferred_element_type=jnp.float32)
        return (out * weight[:, None]).astype(jnp.bfloat16)

    line = jnp.concatenate(ring_gather(my_half(tokens), 1))
    blocks = ring_gather(line, 2)
    half = 2 * rows
    spans = [(0, 0, 4 * rows), (1, 0, 4 * rows), (2, 0, 4 * rows), (3, 0, half), (3, half, 4 * rows)]
    sums = []
    for block, (at, low, high) in zip(blocks, spans):
        other = swap(block)
        back = swap(expert(other, weights_other[at, low:high]))
        sums.append(add(expert(block, weights[at, low:high]), back))

    line_sum = ring_reduce(sums, 2)
    quarter = rows // 2
    pieces = [
        line_sum[0:rows],
        line_sum[rows : 2 * rows],
        line_sum[2 * rows : 3 * rows],
        line_sum[3 * rows : 3 * rows + quarter],
        line_sum[3 * rows + quarter :],
    ]
    plane_sum = ring_reduce(pieces, 1)

    share_rows = rows // n_x
    total = jnp.zeros((share_rows, tokens.shape[1]), jnp.float32)
    for shift in range(n_x):
        at = (x_at + shift) % n_x
        part = lax.dynamic_slice_in_dim(plane_sum, at * share_rows, share_rows, 0)
        total = total + (x_hop(part, shift) if shift else part).astype(jnp.float32)
    share = total.astype(jnp.bfloat16)
    mine = jnp.zeros((rows, tokens.shape[1]), jnp.bfloat16)
    for shift in range(n_x):
        part = x_hop(share, shift) if shift else share
        mine = lax.dynamic_update_slice_in_dim(mine, part, ((x_at - shift) % n_x) * share_rows, 0)
    other = swap(mine)
    mixed = jnp.where(core == 0, jnp.concatenate([mine, other]), jnp.concatenate([other, mine]))
    return (mixed, total_loads)


def solution(mesh):
    torus = Mesh(mesh.devices.reshape(4, 4, mesh.shape["expert"] // 2, 2), ("z", "y", "x", "c"))
    expert = ("x", "c")
    in_specs = (
        P(DP, None),
        P(DP, None),
        P(DP, None),
        P(DP),
        P(expert, None, DP),
        P(expert, None, DP),
        P(expert, DP, None),
    )
    out_specs = (P(DP, None), P())
    return jax.shard_map(per_device, mesh=torus, in_specs=in_specs, out_specs=out_specs, check_vma=False)
```

```python
import functools

import jax
import jax.numpy as jnp
from jax import lax
from jax.experimental import pallas as pl
from jax.experimental.pallas import tpu as pltpu
from jax.sharding import Mesh
from jax.sharding import PartitionSpec as P

DP = ("z", "y")
PLANE = ("z", "y", "c")
LANES = 128


def plane_perm(stage, shift, nz, ny):
    pairs = []
    for z in range(nz):
        for y in range(ny):
            for c in range(2):
                along_y = (stage == 1) == (c == 0)
                to_z, to_y = (z, (y + shift) % ny) if along_y else ((z + shift) % nz, y)
                pairs.append(((z * ny + y) * 2 + c, (to_z * ny + to_y) * 2 + c))
    return pairs


def hop(value, stage, shift):
    perm = plane_perm(stage, shift, lax.axis_size("z"), lax.axis_size("y"))
    return lax.ppermute(value, PLANE, perm)


def swap(value):
    return lax.ppermute(value, "c", [(0, 1), (1, 0)])


def total_of(*parts):
    return sum(part.astype(jnp.float32) for part in parts).astype(jnp.bfloat16)


def ring_reduce(mine, ahead, behind, far_low, far_high, stage):
    a_high = hop(ahead[1], stage, 1)
    b_low = hop(behind[0], stage, -1)
    got_low = hop(far_low, stage, 1)
    got_high = hop(far_high, stage, -1)
    a_low = hop(total_of(ahead[0], got_low), stage, 1)
    b_high = hop(total_of(behind[1], got_high), stage, -1)
    return total_of(mine[0], a_low, b_low), total_of(mine[1], a_high, b_high)


def silu(v):
    return v / (1.0 + jnp.exp(-v))


def expert_kernel(n, width, my_expert, *refs):
    blocks, (gate, up, down), outs, loads = refs[:n], refs[n : n + 3], refs[n + 3 : -1], refs[-1]
    mine = my_expert[0].astype(jnp.float32)
    counted = jnp.zeros((1, LANES), jnp.float32)
    for block, out in zip(blocks, outs):
        x = block[:, :width]
        g = jnp.dot(x, gate[...], preferred_element_type=jnp.float32)
        u = jnp.dot(x, up[...], preferred_element_type=jnp.float32)
        hidden = (silu(g) * u).astype(jnp.bfloat16)
        route = block[:, width:].astype(jnp.float32)
        first, second = route[:, 0:1], route[:, 1:2]
        w_first = route[:, 2:3] + route[:, 3:4] + route[:, 4:5]
        w_second = route[:, 5:6] + route[:, 6:7] + route[:, 7:8]
        w = jnp.where(first == mine, w_first, 0.0) + jnp.where(second == mine, w_second, 0.0)
        lane = lax.broadcasted_iota(jnp.int32, route.shape, 1).astype(jnp.float32)
        named = (lane == first).astype(jnp.float32) + (lane == second).astype(jnp.float32)
        counted = counted + jnp.sum(named, axis=0, keepdims=True)
        step = 1024
        for c in range(0, width, step):
            y = jnp.dot(hidden, down[:, c : c + step], preferred_element_type=jnp.float32)
            out[:, c : c + step] = (y * w).astype(jnp.bfloat16)
    loads[...] = jnp.broadcast_to(counted, loads.shape)


def experts(blocks, my_expert, matrices):
    width, hidden = matrices[0].shape
    flops = 6 * sum(block.shape[0] for block in blocks) * width * hidden
    vmem = pl.BlockSpec(memory_space=pltpu.VMEM)
    blocks = [pltpu.with_memory_space_constraint(block, pltpu.VMEM) for block in blocks]
    *outs, loads = pl.pallas_call(
        functools.partial(expert_kernel, len(blocks), width),
        in_specs=[pl.BlockSpec(memory_space=pltpu.SMEM)] + [vmem] * (len(blocks) + 3),
        out_specs=[vmem] * (len(blocks) + 1),
        out_shape=[jax.ShapeDtypeStruct((block.shape[0], width), jnp.bfloat16) for block in blocks]
        + [jax.ShapeDtypeStruct((8, LANES), jnp.float32)],
        cost_estimate=pl.CostEstimate(flops=flops, bytes_accessed=1 << 24, transcendentals=0),
        compiler_params=pltpu.CompilerParams(vmem_limit_bytes=20 << 20),
        name="experts",
    )(my_expert, *blocks, *matrices)
    return outs, loads


def layer(tokens, expert_ids, gate_weights, live_counts, w_gate, w_up, w_down):
    core = lax.axis_index("c")
    x_at = lax.axis_index("x")
    n_x = lax.axis_size("x")
    my_expert = (x_at * 2 + core).astype(jnp.int32).reshape(1)
    n_experts = n_x * 2
    rows = tokens.shape[0] // 2
    start = core * rows

    def my_half(array):
        return lax.dynamic_slice_in_dim(array, start, rows, 0)

    is_live = start + jnp.arange(rows, dtype=jnp.int32)[:, None] < live_counts[0]
    ids = jnp.where(is_live, my_half(expert_ids), -1).astype(jnp.float32)
    rest = my_half(gate_weights)
    terms = []
    for _ in range(3):
        term = lax.reduce_precision(rest, 8, 7)
        terms.append(term)
        rest = rest - term
    columns = [ids] + [term[:, k : k + 1] for k in range(2) for term in terms]
    columns.append(jnp.zeros((rows, LANES - 8), jnp.float32))
    packed = jnp.concatenate([my_half(tokens)] + [column.astype(jnp.bfloat16) for column in columns], axis=1)

    matrices = tuple(pltpu.with_memory_space_constraint(m[0], pltpu.VMEM) for m in (w_gate, w_up, w_down))
    loads = []

    def run(*blocks):
        outs, counted = experts(blocks, my_expert, matrices)
        loads.append(counted)
        return outs

    line = jnp.concatenate([packed, hop(packed, 1, -1), hop(packed, 1, 1), hop(packed, 1, 2)])
    half = line.shape[0] // 2
    ahead = hop(line, 2, -1)
    behind = hop(line, 2, 1)
    far_low = hop(behind[:half], 2, 1)
    far_high = hop(ahead[half:], 2, -1)

    def joined(own, other):
        back = swap(other)
        return lax.optimization_barrier((total_of(own[:half], back[:half]), total_of(own[half:], back[half:])))

    own, other = run(line, swap(line))
    mine = joined(own, other)
    own, other = run(ahead, swap(ahead))
    ahead = joined(own, other)
    own, other = run(behind, swap(behind))
    behind = joined(own, other)
    shared = swap(far_low), swap(far_high)
    own_low, own_high, low, high = run(far_low, far_high, *shared)
    far_low = total_of(own_low, swap(low))
    far_high = total_of(own_high, swap(high))

    near, further = ring_reduce(mine, ahead, behind, far_low, far_high, 2)
    plane_sum = total_of(
        near[:rows],
        hop(near[rows:], 1, 1),
        hop(further[:rows], 1, -1),
        hop(further[rows:], 1, 2),
    )

    share_rows = rows // n_x
    shares = plane_sum.reshape(n_x, share_rows, -1)
    shares = lax.all_to_all(shares, "x", 0, 0, tiled=True)
    share = jnp.sum(shares.astype(jnp.float32), axis=0).astype(jnp.bfloat16)
    shares = lax.all_to_all(jnp.broadcast_to(share, shares.shape), "x", 0, 0, tiled=True)
    half_out = shares.reshape(rows, -1)
    other = swap(half_out)
    mixed = jnp.where(core == 0, jnp.concatenate([half_out, other]), jnp.concatenate([other, half_out]))
    total_loads = sum(loads)[0, :n_experts].astype(jnp.int32)
    return (mixed, total_loads)


def solution(mesh):
    torus = Mesh(mesh.devices.reshape(4, 4, mesh.shape["expert"] // 2, 2), ("z", "y", "x", "c"))
    expert = ("x", "c")
    in_specs = (
        P(DP, None),
        P(DP, None),
        P(DP, None),
        P(DP),
        P(expert, None, DP),
        P(expert, None, DP),
        P(expert, DP, None),
    )
    out_specs = (P(DP, None), P())
    return jax.shard_map(layer, mesh=torus, in_specs=in_specs, out_specs=out_specs, check_vma=False)
```

```python
import functools

import jax
import jax.numpy as jnp
from jax import lax
from jax.experimental import pallas as pl
from jax.experimental.pallas import tpu as pltpu
from jax.sharding import Mesh
from jax.sharding import PartitionSpec as P

DP = ("z", "y")
PLANE = ("z", "y", "c")
LANES = 128
STEP = 1024


def plane_perm(stage, shift, nz, ny):
    pairs = []
    for z in range(nz):
        for y in range(ny):
            for c in range(2):
                along_y = (stage == 1) == (c == 0)
                to_z, to_y = (z, (y + shift) % ny) if along_y else ((z + shift) % nz, y)
                pairs.append(((z * ny + y) * 2 + c, (to_z * ny + to_y) * 2 + c))
    return pairs


def hop(value, stage, shift):
    perm = plane_perm(stage, shift, lax.axis_size("z"), lax.axis_size("y"))
    return lax.ppermute(value, PLANE, perm)


def swap(value):
    return lax.ppermute(value, "c", [(0, 1), (1, 0)])


def total_of(*parts):
    return sum(part.astype(jnp.float32) for part in parts).astype(jnp.bfloat16)


def silu(v):
    return v / (1.0 + jnp.exp(-v))


def expert_kernel(n, width, my_expert, *refs):
    blocks, (gate, up, down), outs, loads = refs[:n], refs[n : n + 3], refs[n + 3 : 2 * n + 3], refs[2 * n + 3]
    hidden, weight = refs[2 * n + 4 :]
    mine = my_expert[0].astype(jnp.float32)
    counted = jnp.zeros((1, LANES), jnp.float32)
    rows = blocks[0].shape[0]
    for i, block in enumerate(blocks):
        x = block[:, :width]
        g = jnp.dot(x, gate[...], preferred_element_type=jnp.float32)
        u = jnp.dot(x, up[...], preferred_element_type=jnp.float32)
        hidden[i * rows : (i + 1) * rows] = (silu(g) * u).astype(jnp.bfloat16)
        route = block[:, width:].astype(jnp.float32)
        first, second = route[:, 0:1], route[:, 1:2]
        w_first = route[:, 2:3] + route[:, 3:4] + route[:, 4:5]
        w_second = route[:, 5:6] + route[:, 6:7] + route[:, 7:8]
        w = jnp.where(first == mine, w_first, 0.0) + jnp.where(second == mine, w_second, 0.0)
        weight[i * rows : (i + 1) * rows] = jnp.broadcast_to(w, (rows, LANES))
        lane = lax.broadcasted_iota(jnp.int32, route.shape, 1).astype(jnp.float32)
        named = (lane == first).astype(jnp.float32) + (lane == second).astype(jnp.float32)
        counted = counted + jnp.sum(named, axis=0, keepdims=True)
    loads[...] = jnp.broadcast_to(counted, loads.shape)

    def columns(k, _):
        at = pl.ds(pl.multiple_of(k * STEP, STEP), STEP)
        y = jnp.dot(hidden[...], down[:, at], preferred_element_type=jnp.float32)
        y = (y * weight[:, :1]).astype(jnp.bfloat16)
        for i, out in enumerate(outs):
            out[:, at] = y[i * rows : (i + 1) * rows]
        return 0

    lax.fori_loop(0, width // STEP, columns, 0)


def experts(blocks, my_expert, matrices):
    width, hidden = matrices[0].shape
    flops = 6 * sum(block.shape[0] for block in blocks) * width * hidden
    vmem = pl.BlockSpec(memory_space=pltpu.VMEM)
    blocks = [pltpu.with_memory_space_constraint(block, pltpu.VMEM) for block in blocks]
    *outs, loads = pl.pallas_call(
        functools.partial(expert_kernel, len(blocks), width),
        in_specs=[pl.BlockSpec(memory_space=pltpu.SMEM)] + [vmem] * (len(blocks) + 3),
        out_specs=[vmem] * (len(blocks) + 1),
        out_shape=[jax.ShapeDtypeStruct((block.shape[0], width), jnp.bfloat16) for block in blocks]
        + [jax.ShapeDtypeStruct((8, LANES), jnp.float32)],
        scratch_shapes=[
            pltpu.VMEM((sum(block.shape[0] for block in blocks), hidden), jnp.bfloat16),
            pltpu.VMEM((sum(block.shape[0] for block in blocks), LANES), jnp.float32),
        ],
        cost_estimate=pl.CostEstimate(flops=flops, bytes_accessed=1 << 24, transcendentals=0),
        compiler_params=pltpu.CompilerParams(vmem_limit_bytes=20 << 20),
        name="experts",
    )(my_expert, *blocks, *matrices)
    return outs, loads


def pack(tokens, expert_ids, gate_weights, live_counts, start):
    count, width = tokens.shape
    rows = count // 2

    def kernel(live, first, tokens, ids, gates, out):
        at = pl.ds(pl.multiple_of(first[0], rows), rows)
        out[:, :width] = tokens[at, :]
        place = lax.broadcasted_iota(jnp.int32, (2, count), 1)
        lines = [jnp.where(place < live[0], ids[...], -1).astype(jnp.float32)]
        rest, terms = gates[...], []
        for _ in range(3):
            terms.append(rest.astype(jnp.bfloat16).astype(jnp.float32))
            rest = rest - terms[-1]
        lines += [term[k : k + 1] for k in range(2) for term in terms]
        lines.append(jnp.zeros((LANES - 8, count), jnp.float32))
        columns = jnp.concatenate(lines, axis=0).T
        low, high = columns[:rows], columns[rows:]
        out[:, width:] = jnp.where(first[0] == 0, low, high).astype(jnp.bfloat16)

    smem, vmem = pl.BlockSpec(memory_space=pltpu.SMEM), pl.BlockSpec(memory_space=pltpu.VMEM)
    return pl.pallas_call(
        kernel,
        in_specs=[smem, smem, vmem, vmem, vmem],
        out_specs=vmem,
        out_shape=jax.ShapeDtypeStruct((rows, width + LANES), jnp.bfloat16),
        compiler_params=pltpu.CompilerParams(vmem_limit_bytes=8 << 20),
        name="pack",
    )(live_counts, start.astype(jnp.int32).reshape(1), tokens, expert_ids.T, gate_weights.T)


def staged(my_expert, matrices):
    def kernel(expert, gate, up, down, out):
        out[0] = expert[0]

    smem, vmem = pl.BlockSpec(memory_space=pltpu.SMEM), pl.BlockSpec(memory_space=pltpu.VMEM)
    return pl.pallas_call(
        kernel,
        in_specs=[smem, vmem, vmem, vmem],
        out_specs=smem,
        out_shape=jax.ShapeDtypeStruct((1,), jnp.int32),
        compiler_params=pltpu.CompilerParams(vmem_limit_bytes=1 << 20),
        name="stage",
    )(my_expert, *matrices)


def layer(tokens, expert_ids, gate_weights, live_counts, w_gate, w_up, w_down):
    core = lax.axis_index("c")
    x_at = lax.axis_index("x")
    n_x = lax.axis_size("x")
    my_expert = (x_at * 2 + core).astype(jnp.int32).reshape(1)
    n_experts = n_x * 2
    rows = tokens.shape[0] // 2
    start = core * rows

    matrices = tuple(pltpu.with_memory_space_constraint(m[0], pltpu.VMEM) for m in (w_gate, w_up, w_down))
    packed = pack(tokens, expert_ids, gate_weights, live_counts, start)
    loads = []

    my_expert = staged(my_expert, matrices)
    low = jnp.concatenate([packed, hop(packed, 1, -1)])
    high = jnp.concatenate([hop(packed, 1, 1), hop(packed, 1, 2)])
    behind_low = hop(low, 2, 1)
    ahead_high = hop(high, 2, -1)
    ahead_low = hop(low, 2, -1)
    behind_high = hop(high, 2, 1)
    far_low = hop(behind_low, 2, 1)
    far_high = hop(ahead_high, 2, -1)

    def run(*blocks):
        shared = [swap(block) for block in blocks]
        outs, counted = experts((*blocks, *shared), my_expert, matrices)
        loads.append(counted)
        mine, others = outs[: len(blocks)], outs[len(blocks) :]
        back = [swap(other) for other in others]
        return lax.optimization_barrier([total_of(*pair) for pair in zip(mine, back)])

    low, high = run(low, high)
    behind_low, ahead_high = run(behind_low, ahead_high)
    ahead_low, behind_high = run(ahead_low, behind_high)
    far_low, far_high = run(far_low, far_high)

    from_ahead_low = hop(behind_low, 2, -1)
    from_behind_high = hop(ahead_high, 2, 1)
    from_behind_low = hop(ahead_low, 2, 1)
    from_ahead_high = hop(behind_high, 2, -1)
    from_far_low = hop(far_low, 2, 2)
    from_far_high = hop(far_high, 2, 2)
    near = total_of(low, from_ahead_low, from_behind_low, from_far_low)
    further = total_of(high, from_ahead_high, from_behind_high, from_far_high)
    plane_sum = total_of(
        near[:rows],
        hop(near[rows:], 1, 1),
        hop(further[:rows], 1, -1),
        hop(further[rows:], 1, 2),
    )

    share_rows = rows // n_x
    shares = plane_sum.reshape(n_x, share_rows, -1)
    shares = lax.all_to_all(shares, "x", 0, 0, tiled=True)
    share = jnp.sum(shares.astype(jnp.float32), axis=0).astype(jnp.bfloat16)
    shares = lax.all_to_all(jnp.broadcast_to(share, shares.shape), "x", 0, 0, tiled=True)
    half_out = shares.reshape(rows, -1)
    other = swap(half_out)
    mixed = jnp.where(core == 0, jnp.concatenate([half_out, other]), jnp.concatenate([other, half_out]))
    total_loads = sum(loads)[0, :n_experts].astype(jnp.int32)
    return (mixed, total_loads)


def solution(mesh):
    torus = Mesh(mesh.devices.reshape(4, 4, mesh.shape["expert"] // 2, 2), ("z", "y", "x", "c"))
    expert = ("x", "c")
    in_specs = (
        P(DP, None),
        P(DP, None),
        P(DP, None),
        P(DP),
        P(expert, None, DP),
        P(expert, None, DP),
        P(expert, DP, None),
    )
    out_specs = (P(DP, None), P())
    return jax.shard_map(layer, mesh=torus, in_specs=in_specs, out_specs=out_specs, check_vma=False)
```

```python
import functools

import jax
import jax.numpy as jnp
from jax import lax
from jax.experimental import pallas as pl
from jax.experimental.pallas import tpu as pltpu
from jax.sharding import Mesh
from jax.sharding import PartitionSpec as P

DP = ("z", "y")
PLANE = ("z", "y", "c")
LANES = 128
STEP = 1024


def plane_perm(stage, shift, nz, ny):
    pairs = []
    for z in range(nz):
        for y in range(ny):
            for c in range(2):
                along_y = (stage == 1) == (c == 0)
                to_z, to_y = (z, (y + shift) % ny) if along_y else ((z + shift) % nz, y)
                pairs.append(((z * ny + y) * 2 + c, (to_z * ny + to_y) * 2 + c))
    return pairs


def hop(value, stage, shift):
    perm = plane_perm(stage, shift, lax.axis_size("z"), lax.axis_size("y"))
    return lax.ppermute(value, PLANE, perm)


def swap(value):
    return lax.ppermute(value, "c", [(0, 1), (1, 0)])


def x_hop(value, shift):
    size = lax.axis_size("x")
    return lax.ppermute(value, "x", [(i, (i + shift) % size) for i in range(size)])


def total_of(*parts):
    return sum(part.astype(jnp.float32) for part in parts).astype(jnp.bfloat16)


def silu(v):
    return v / (1.0 + jnp.exp(-v))


def expert_kernel(n, width, rolled, my_expert, *refs):
    blocks, (gate, up, down), outs, loads = refs[:n], refs[n : n + 3], refs[n + 3 : 2 * n + 3], refs[2 * n + 3]
    hidden = refs[2 * n + 4]
    units = hidden.shape[1]

    def expand(at):
        x = jnp.concatenate([block[:, :width] for block in blocks])
        g = jnp.dot(x, gate[:, at], preferred_element_type=jnp.float32)
        u = jnp.dot(x, up[:, at], preferred_element_type=jnp.float32)
        return (silu(g) * u).astype(jnp.bfloat16)

    if rolled:
        part = units // 2

        def step(k, _):
            at = pl.ds(pl.multiple_of(k * part, part), part)
            hidden[:, at] = expand(at)
            return 0

        lax.fori_loop(0, 2, step, 0)
        held = hidden[...]
    else:
        held = expand(slice(0, units))

    mine = my_expert[0].astype(jnp.float32)
    route = jnp.concatenate([block[:, width:] for block in blocks]).astype(jnp.float32)
    first, second = route[:, 0:1], route[:, 1:2]
    w_first = route[:, 2:3] + route[:, 3:4] + route[:, 4:5]
    w_second = route[:, 5:6] + route[:, 6:7] + route[:, 7:8]
    w = jnp.where(first == mine, w_first, 0.0) + jnp.where(second == mine, w_second, 0.0)
    lane = lax.broadcasted_iota(jnp.int32, route.shape, 1).astype(jnp.float32)
    named = (lane == first).astype(jnp.float32) + (lane == second).astype(jnp.float32)
    loads[...] = jnp.broadcast_to(jnp.sum(named, axis=0, keepdims=True), loads.shape)
    for c in range(0, width, STEP):
        y = jnp.dot(held, down[:, c : c + STEP], preferred_element_type=jnp.float32)
        y = (y * w).astype(jnp.bfloat16)
        at = 0
        for block, out in zip(blocks, outs):
            out[:, c : c + STEP] = y[at : at + block.shape[0]]
            at += block.shape[0]


def experts(blocks, my_expert, matrices, rolled):
    width, hidden = matrices[0].shape
    flops = 6 * sum(block.shape[0] for block in blocks) * width * hidden
    vmem = pl.BlockSpec(memory_space=pltpu.VMEM)
    blocks = [pltpu.with_memory_space_constraint(block, pltpu.VMEM) for block in blocks]
    *outs, loads = pl.pallas_call(
        functools.partial(expert_kernel, len(blocks), width, rolled),
        in_specs=[pl.BlockSpec(memory_space=pltpu.SMEM)] + [vmem] * (len(blocks) + 3),
        out_specs=[vmem] * (len(blocks) + 1),
        out_shape=[jax.ShapeDtypeStruct((block.shape[0], width), jnp.bfloat16) for block in blocks]
        + [jax.ShapeDtypeStruct((8, LANES), jnp.float32)],
        scratch_shapes=[pltpu.VMEM((sum(block.shape[0] for block in blocks), hidden), jnp.bfloat16)],
        cost_estimate=pl.CostEstimate(flops=flops, bytes_accessed=1 << 24, transcendentals=0),
        compiler_params=pltpu.CompilerParams(vmem_limit_bytes=20 << 20),
        name="experts",
    )(my_expert, *blocks, *matrices)
    return outs, loads


def pack(tokens, expert_ids, gate_weights, live_counts, start):
    count, width = tokens.shape
    rows = count // 2

    def kernel(live, first, tokens, ids, gates, out):
        at = pl.ds(pl.multiple_of(first[0], rows), rows)
        out[:, :width] = tokens[at, :]
        place = lax.broadcasted_iota(jnp.int32, (2, count), 1)
        lines = [jnp.where(place < live[0], ids[...], -1).astype(jnp.float32)]
        rest, terms = gates[...], []
        for _ in range(3):
            terms.append(rest.astype(jnp.bfloat16).astype(jnp.float32))
            rest = rest - terms[-1]
        lines += [term[k : k + 1] for k in range(2) for term in terms]
        lines.append(jnp.zeros((LANES - 8, count), jnp.float32))
        columns = jnp.concatenate(lines, axis=0).T
        low, high = columns[:rows], columns[rows:]
        out[:, width:] = jnp.where(first[0] == 0, low, high).astype(jnp.bfloat16)

    smem, vmem = pl.BlockSpec(memory_space=pltpu.SMEM), pl.BlockSpec(memory_space=pltpu.VMEM)
    return pl.pallas_call(
        kernel,
        in_specs=[smem, smem, vmem, vmem, vmem],
        out_specs=vmem,
        out_shape=jax.ShapeDtypeStruct((rows, width + LANES), jnp.bfloat16),
        compiler_params=pltpu.CompilerParams(vmem_limit_bytes=8 << 20),
        name="pack",
    )(live_counts, start.astype(jnp.int32).reshape(1), tokens, expert_ids.T, gate_weights.T)


def staged(my_expert, matrices):
    def kernel(expert, gate, up, down, out):
        out[0] = expert[0]

    smem, vmem = pl.BlockSpec(memory_space=pltpu.SMEM), pl.BlockSpec(memory_space=pltpu.VMEM)
    return pl.pallas_call(
        kernel,
        in_specs=[smem, vmem, vmem, vmem],
        out_specs=smem,
        out_shape=jax.ShapeDtypeStruct((1,), jnp.int32),
        compiler_params=pltpu.CompilerParams(vmem_limit_bytes=1 << 20),
        name="stage",
    )(my_expert, *matrices)


def layer(tokens, expert_ids, gate_weights, live_counts, w_gate, w_up, w_down):
    core = lax.axis_index("c")
    x_at = lax.axis_index("x")
    n_x = lax.axis_size("x")
    my_expert = (x_at * 2 + core).astype(jnp.int32).reshape(1)
    n_experts = n_x * 2
    rows = tokens.shape[0] // 2
    start = core * rows

    matrices = tuple(pltpu.with_memory_space_constraint(m[0], pltpu.VMEM) for m in (w_gate, w_up, w_down))
    packed = pack(tokens, expert_ids, gate_weights, live_counts, start)
    loads = []

    my_expert = staged(my_expert, matrices)
    low = jnp.concatenate([packed, hop(packed, 1, 2)])
    high = jnp.concatenate([hop(packed, 1, -1), hop(packed, 1, 1)])
    behind_low = hop(low, 2, 1)
    ahead_high = hop(high, 2, -1)
    ahead_low = hop(low, 2, -1)
    behind_high = hop(high, 2, 1)
    far_low = hop(behind_low, 2, 1)
    far_high = hop(ahead_high, 2, -1)

    def run(name, *blocks):
        shared = [swap(block) for block in blocks]
        if name == "mine":
            outs, counted = experts((*blocks, *shared), my_expert, matrices, True)
            loads.append(counted)
            mine, others = outs[: len(blocks)], outs[len(blocks) :]
        else:
            others, counted = experts(shared, my_expert, matrices, name == "first")
            loads.append(counted)
            mine, counted = experts(blocks, my_expert, matrices, name == "first")
            loads.append(counted)
        back = [swap(other) for other in others]
        return lax.optimization_barrier([total_of(*pair) for pair in zip(mine, back)])

    low, high = run("mine", low, high)
    behind_low, ahead_high = run("first", behind_low, ahead_high)
    ahead_low, behind_high = run("second", ahead_low, behind_high)
    far_low, far_high = run("far", far_low, far_high)

    from_ahead_low = hop(behind_low, 2, -1)
    from_behind_high = hop(ahead_high, 2, 1)
    from_behind_low = hop(ahead_low, 2, 1)
    from_ahead_high = hop(behind_high, 2, -1)
    from_far_low = hop(far_low, 2, 2)
    from_far_high = hop(far_high, 2, 2)
    near = total_of(low, from_ahead_low, from_behind_low, from_far_low)
    further = total_of(high, from_ahead_high, from_behind_high, from_far_high)
    plane_sum = total_of(
        near[:rows],
        hop(near[rows:], 1, 2),
        hop(further[:rows], 1, 1),
        hop(further[rows:], 1, -1),
    )

    share_rows = rows // n_x
    parts = []
    for shift in range(n_x):
        at = (x_at + shift) % n_x
        part = lax.dynamic_slice_in_dim(plane_sum, at * share_rows, share_rows, 0)
        parts.append(x_hop(part, shift) if shift else part)
    share = total_of(*parts)
    half_out = jnp.zeros(plane_sum.shape, jnp.bfloat16)
    for shift in range(n_x):
        part = x_hop(share, shift) if shift else share
        half_out = lax.dynamic_update_slice_in_dim(half_out, part, ((x_at - shift) % n_x) * share_rows, 0)
    other = swap(half_out)
    mixed = jnp.where(core == 0, jnp.concatenate([half_out, other]), jnp.concatenate([other, half_out]))
    total_loads = sum(loads)[0, :n_experts].astype(jnp.int32)
    return (mixed, total_loads)


def solution(mesh):
    torus = Mesh(mesh.devices.reshape(4, 4, mesh.shape["expert"] // 2, 2), ("z", "y", "x", "c"))
    expert = ("x", "c")
    in_specs = (
        P(DP, None),
        P(DP, None),
        P(DP, None),
        P(DP),
        P(expert, None, DP),
        P(expert, None, DP),
        P(expert, DP, None),
    )
    out_specs = (P(DP, None), P())
    return jax.shard_map(layer, mesh=torus, in_specs=in_specs, out_specs=out_specs, check_vma=False)
```

```python
import functools

import jax
import jax.numpy as jnp
from jax import lax
from jax.experimental import pallas as pl
from jax.experimental.pallas import tpu as pltpu
from jax.sharding import Mesh
from jax.sharding import PartitionSpec as P

DP = ("z", "y")
PLANE = ("z", "y", "c")
LANES = 128
STEP = 1024


def plane_perm(stage, shift, nz, ny):
    pairs = []
    for z in range(nz):
        for y in range(ny):
            for c in range(2):
                along_y = (stage == 1) == (c == 1)
                to_z, to_y = (z, (y + shift) % ny) if along_y else ((z + shift) % nz, y)
                pairs.append(((z * ny + y) * 2 + c, (to_z * ny + to_y) * 2 + c))
    return pairs


def hop(value, stage, shift):
    perm = plane_perm(stage, shift, lax.axis_size("z"), lax.axis_size("y"))
    return lax.ppermute(value, PLANE, perm)


def swap(value):
    return lax.ppermute(value, "c", [(0, 1), (1, 0)])


def x_hop(value, shift):
    size = lax.axis_size("x")
    return lax.ppermute(value, "x", [(i, (i + shift) % size) for i in range(size)])


def total_of(*parts):
    return sum(part.astype(jnp.float32) for part in parts).astype(jnp.bfloat16)


def silu(v):
    return v / (1.0 + jnp.exp(-v))


def expert_kernel(n, width, rolled, my_expert, *refs):
    blocks, (gate, up, down), outs, loads = refs[:n], refs[n : n + 3], refs[n + 3 : 2 * n + 3], refs[2 * n + 3]
    hidden = refs[2 * n + 4]
    units = hidden.shape[1]

    def expand(at):
        x = jnp.concatenate([block[:, :width] for block in blocks])
        g = jnp.dot(x, gate[:, at], preferred_element_type=jnp.float32)
        u = jnp.dot(x, up[:, at], preferred_element_type=jnp.float32)
        return (silu(g) * u).astype(jnp.bfloat16)

    if rolled:
        part = units // 2

        def step(k, _):
            at = pl.ds(pl.multiple_of(k * part, part), part)
            hidden[:, at] = expand(at)
            return 0

        lax.fori_loop(0, 2, step, 0)
        held = hidden[...]
    else:
        held = expand(slice(0, units))

    mine = my_expert[0].astype(jnp.float32)
    route = jnp.concatenate([block[:, width:] for block in blocks]).astype(jnp.float32)
    first, second = route[:, 0:1], route[:, 1:2]
    w_first = route[:, 2:3] + route[:, 3:4] + route[:, 4:5]
    w_second = route[:, 5:6] + route[:, 6:7] + route[:, 7:8]
    w = jnp.where(first == mine, w_first, 0.0) + jnp.where(second == mine, w_second, 0.0)
    lane = lax.broadcasted_iota(jnp.int32, route.shape, 1).astype(jnp.float32)
    named = (lane == first).astype(jnp.float32) + (lane == second).astype(jnp.float32)
    loads[...] = jnp.broadcast_to(jnp.sum(named, axis=0, keepdims=True), loads.shape)
    for c in range(0, width, STEP):
        y = jnp.dot(held, down[:, c : c + STEP], preferred_element_type=jnp.float32)
        y = (y * w).astype(jnp.bfloat16)
        at = 0
        for block, out in zip(blocks, outs):
            out[:, c : c + STEP] = y[at : at + block.shape[0]]
            at += block.shape[0]


def experts(blocks, my_expert, matrices, rolled):
    width, hidden = matrices[0].shape
    flops = 6 * sum(block.shape[0] for block in blocks) * width * hidden
    vmem = pl.BlockSpec(memory_space=pltpu.VMEM)
    blocks = [pltpu.with_memory_space_constraint(block, pltpu.VMEM) for block in blocks]
    *outs, loads = pl.pallas_call(
        functools.partial(expert_kernel, len(blocks), width, rolled),
        in_specs=[pl.BlockSpec(memory_space=pltpu.SMEM)] + [vmem] * (len(blocks) + 3),
        out_specs=[vmem] * (len(blocks) + 1),
        out_shape=[jax.ShapeDtypeStruct((block.shape[0], width), jnp.bfloat16) for block in blocks]
        + [jax.ShapeDtypeStruct((8, LANES), jnp.float32)],
        scratch_shapes=[pltpu.VMEM((sum(block.shape[0] for block in blocks), hidden), jnp.bfloat16)],
        cost_estimate=pl.CostEstimate(flops=flops, bytes_accessed=1 << 24, transcendentals=0),
        compiler_params=pltpu.CompilerParams(vmem_limit_bytes=10 << 20),
        name="experts",
    )(my_expert, *blocks, *matrices)
    return outs, loads


def small_call(kernel, out_shapes, scalar, *arrays):
    smem, vmem = pl.BlockSpec(memory_space=pltpu.SMEM), pl.BlockSpec(memory_space=pltpu.VMEM)
    return pl.pallas_call(
        kernel,
        in_specs=[smem] + [vmem] * len(arrays),
        out_specs=[vmem] * len(out_shapes),
        out_shape=[jax.ShapeDtypeStruct(shape, jnp.bfloat16) for shape in out_shapes],
        compiler_params=pltpu.CompilerParams(vmem_limit_bytes=10 << 20),
    )(scalar, *arrays)


def add_all(arrays):
    def kernel(_, *refs):
        total = refs[0][...].astype(jnp.float32)
        for ref in refs[1:-1]:
            total = total + ref[...].astype(jnp.float32)
        refs[-1][...] = total.astype(jnp.bfloat16)

    return small_call(kernel, [arrays[0].shape], jnp.zeros((1,), jnp.int32), *arrays)[0]


def split_far(mine, back, x_here, n_x):
    count, width = mine[0].shape
    rows = count // 2
    part = rows // n_x

    def kernel(x, mine_low, mine_high, back_low, back_high, low, high, *shares):
        def add(a, b, at):
            return (a[at, :].astype(jnp.float32) + b[at, :].astype(jnp.float32)).astype(jnp.bfloat16)

        for k, share in enumerate(shares):
            at = rows + lax.rem(x[0] + k, n_x) * part
            share[...] = add(mine_high, back_high, pl.ds(pl.multiple_of(at, part), part))
        low[...] = add(mine_low, back_low, slice(None))
        high[...] = add(mine_high, back_high, slice(0, rows))

    shapes = [(count, width), (rows, width)] + [(part, width)] * n_x
    return small_call(kernel, shapes, x_here, *mine, *back)


def join_low(*arrays):
    count, width = arrays[0].shape
    rows = count // 2

    def kernel(_, *refs):
        for k, out in enumerate(refs[-2:]):
            at = slice(k * rows, (k + 1) * rows)
            out[...] = sum(ref[at, :].astype(jnp.float32) for ref in refs[:-2]).astype(jnp.bfloat16)

    return small_call(kernel, [(rows, width)] * 2, jnp.zeros((1,), jnp.int32), *arrays)


def plane_shares(arrays, x_here, n_x):
    count, width = arrays[0].shape
    part = count // n_x

    def kernel(x, *refs):
        for k, out in enumerate(refs[-n_x:]):
            at = pl.ds(pl.multiple_of(lax.rem(x[0] + k, n_x) * part, part), part)
            out[...] = sum(ref[at, :].astype(jnp.float32) for ref in refs[:-n_x]).astype(jnp.bfloat16)

    return small_call(kernel, [(part, width)] * n_x, x_here, *arrays)


def join_high(high, ahead, behind, far, share, x_here):
    count, width = high.shape
    rows, part = count // 2, share.shape[0]

    def kernel(x, high, ahead, behind, far, share, first, second):
        def add(at):
            total = high[at, :].astype(jnp.float32) + ahead[at, :].astype(jnp.float32)
            return total + behind[at, :].astype(jnp.float32)

        first[...] = (add(slice(0, rows)) + far[...].astype(jnp.float32)).astype(jnp.bfloat16)
        for k in range(rows // part):
            mine = jnp.where(x[0] == k, share[...].astype(jnp.float32), 0.0)
            at = slice(rows + k * part, rows + (k + 1) * part)
            second[k * part : (k + 1) * part] = (add(at) + mine).astype(jnp.bfloat16)

    return small_call(kernel, [(rows, width)] * 2, x_here, high, ahead, behind, far, share)


def pack(tokens, expert_ids, gate_weights, live_counts, start):
    count, width = tokens.shape
    rows = count // 2

    def kernel(live, first, tokens, ids, gates, out):
        at = pl.ds(pl.multiple_of(first[0], rows), rows)
        out[:, :width] = tokens[at, :]
        place = lax.broadcasted_iota(jnp.int32, (2, count), 1)
        lines = [jnp.where(place < live[0], ids[...], -1).astype(jnp.float32)]
        rest, terms = gates[...], []
        for _ in range(3):
            terms.append(rest.astype(jnp.bfloat16).astype(jnp.float32))
            rest = rest - terms[-1]
        lines += [term[k : k + 1] for k in range(2) for term in terms]
        lines.append(jnp.zeros((LANES - 8, count), jnp.float32))
        columns = jnp.concatenate(lines, axis=0).T
        low, high = columns[:rows], columns[rows:]
        out[:, width:] = jnp.where(first[0] == 0, low, high).astype(jnp.bfloat16)

    smem, vmem = pl.BlockSpec(memory_space=pltpu.SMEM), pl.BlockSpec(memory_space=pltpu.VMEM)
    return pl.pallas_call(
        kernel,
        in_specs=[smem, smem, vmem, vmem, vmem],
        out_specs=vmem,
        out_shape=jax.ShapeDtypeStruct((rows, width + LANES), jnp.bfloat16),
        compiler_params=pltpu.CompilerParams(vmem_limit_bytes=8 << 20),
        name="pack",
    )(live_counts, start.astype(jnp.int32).reshape(1), tokens, expert_ids.T, gate_weights.T)


def staged(my_expert, matrices):
    def kernel(expert, gate, up, down, out):
        out[0] = expert[0]

    smem, vmem = pl.BlockSpec(memory_space=pltpu.SMEM), pl.BlockSpec(memory_space=pltpu.VMEM)
    return pl.pallas_call(
        kernel,
        in_specs=[smem, vmem, vmem, vmem],
        out_specs=smem,
        out_shape=jax.ShapeDtypeStruct((1,), jnp.int32),
        compiler_params=pltpu.CompilerParams(vmem_limit_bytes=1 << 20),
        name="stage",
    )(my_expert, *matrices)


def layer(tokens, expert_ids, gate_weights, live_counts, w_gate, w_up, w_down):
    core = lax.axis_index("c")
    x_at = lax.axis_index("x")
    n_x = lax.axis_size("x")
    x_here = x_at.astype(jnp.int32).reshape(1)
    my_expert = (x_at * 2 + core).astype(jnp.int32).reshape(1)
    n_experts = n_x * 2
    rows = tokens.shape[0] // 2
    start = core * rows

    matrices = tuple(pltpu.with_memory_space_constraint(m[0], pltpu.VMEM) for m in (w_gate, w_up, w_down))
    packed = pack(tokens, expert_ids, gate_weights, live_counts, start)
    loads = []

    my_expert = staged(my_expert, matrices)
    low = jnp.concatenate([packed, hop(packed, 1, 2)])
    high = jnp.concatenate([hop(packed, 1, -1), hop(packed, 1, 1)])
    behind_low = hop(low, 2, 1)
    ahead_high = hop(high, 2, -1)
    ahead_low = hop(low, 2, -1)
    behind_high = hop(high, 2, 1)
    far_low = hop(behind_low, 2, 1)
    far_high = hop(ahead_high, 2, -1)

    def run(name, *blocks):
        shared = [swap(block) for block in blocks]
        if name == "mine":
            outs, counted = experts((*blocks, *shared), my_expert, matrices, True)
            loads.append(counted)
            mine, others = outs[: len(blocks)], outs[len(blocks) :]
        else:
            others, counted = experts(shared, my_expert, matrices, name != "far")
            loads.append(counted)
            mine, counted = experts(blocks, my_expert, matrices, name != "far")
            loads.append(counted)
        back = [swap(other) for other in others]
        if name == "far":
            return split_far(mine, back, x_here, n_x)
        return lax.optimization_barrier([total_of(*pair) for pair in zip(mine, back)])

    low, high = run("mine", low, high)
    behind_low, ahead_high = run("first", behind_low, ahead_high)
    ahead_low, behind_high = run("second", ahead_low, behind_high)
    far_low, far_high, *shares = run("far", far_low, far_high)

    from_ahead_low = hop(behind_low, 2, -1)
    from_behind_high = hop(ahead_high, 2, 1)
    from_behind_low = hop(ahead_low, 2, 1)
    from_ahead_high = hop(behind_high, 2, -1)
    shares = shares[:1] + [x_hop(shares[shift], shift) for shift in range(1, n_x)]
    share = hop(add_all(shares), 2, 2)
    from_far_low = hop(far_low, 2, 2)
    from_far_high = hop(far_high, 2, 2)
    near = join_low(low, from_ahead_low, from_behind_low, from_far_low)
    lines = [near[0], hop(near[1], 1, 2)]
    further = join_high(high, from_ahead_high, from_behind_high, from_far_high, share, x_here)
    lines += [hop(further[0], 1, 1), hop(further[1], 1, -1)]

    shares = list(plane_shares(lines, x_here, n_x))
    share = add_all(shares[:1] + [x_hop(shares[shift], shift) for shift in range(1, n_x)])
    share_rows = share.shape[0]
    half_out = jnp.zeros(lines[0].shape, jnp.bfloat16)
    for shift in range(n_x):
        part = x_hop(share, shift) if shift else share
        half_out = lax.dynamic_update_slice_in_dim(half_out, part, ((x_at - shift) % n_x) * share_rows, 0)
    other = swap(half_out)
    mixed = jnp.where(core == 0, jnp.concatenate([half_out, other]), jnp.concatenate([other, half_out]))
    total_loads = sum(loads)[0, :n_experts].astype(jnp.int32)
    return (mixed, total_loads)


def solution(mesh):
    torus = Mesh(mesh.devices.reshape(4, 4, mesh.shape["expert"] // 2, 2), ("z", "y", "x", "c"))
    expert = ("x", "c")
    in_specs = (
        P(DP, None),
        P(DP, None),
        P(DP, None),
        P(DP),
        P(expert, None, DP),
        P(expert, None, DP),
        P(expert, DP, None),
    )
    out_specs = (P(DP, None), P())
    return jax.shard_map(layer, mesh=torus, in_specs=in_specs, out_specs=out_specs, check_vma=False)
```
